512 devices in a mesh: dp: 64 (over z_hi, y, core), mp: 8 (over x, z_lo).
Axes of the slice: x: 4, y: 8, z: 8 (z_hi: 4, z_lo: 2; z = z_hi * 2 + z_lo), core: 2. Of those that a mesh axis runs over, the one named last changes fastest.
Arguments:
- features: bfloat16 [3072, 384], P('dp'), may hold values from -100 to 100
- teacher_weight: float32 [384, 131072], P(None, ('dp', 'mp')), may hold values from -250 to 250
- student_weight: float32 [384, 131072], P(None, ('dp', 'mp')), may hold values from -24 to 24
- center: float32 [131072], P(('dp', 'mp')), may hold values from -1 to 1
Outputs:
- blended: float32 [384, 131072], P(None, ('dp', 'mp'))
- new_center: float32 [131072], P(('dp', 'mp'))
- log_targets: float32 [3072, 131072], P(None, ('dp', 'mp'))
The draws below stay inside these ranges and needn't reach their ends.
All inputs are finite; a program needn't handle non-finite values.
Results may differ from the reference program's by a relative error of at most 0.0003.
Values may be sent and summed in bfloat16 or wider, within the bound.
A program may use at most 64 MiB of HBM per device.

```python
import math
import jax
import jax.numpy as jnp
from jax import lax

D = 384
K = 131072
IMAGES = 3072


def mean_direction(key):
    return jax.random.normal(jax.random.fold_in(key, 101), (D,), jnp.float32)


def draw_features(key, part):
    shared = mean_direction(key)
    jitter_key, scale_key = jax.random.split(jax.random.fold_in(key, 202))
    jitter = jax.random.normal(jitter_key, (IMAGES, D), jnp.float32)
    scales = jnp.exp(jax.random.uniform(scale_key, (IMAGES, 1), jnp.float32) * math.log(10.0))
    return jnp.clip((shared[None, :] + jitter) * scales, -100.0, 100.0).astype(jnp.bfloat16)


def draw_teacher_weight(key, part):
    shared = mean_direction(key)
    jitter_key, align_key, scale_key = jax.random.split(jax.random.fold_in(key, 303), 3)
    jitter = jax.random.normal(jitter_key, (D, K), jnp.float32)
    alignment = 0.6 * jax.random.normal(align_key, (1, K), jnp.float32)
    scales = jnp.exp(jax.random.uniform(scale_key, (1, K), jnp.float32) * math.log(10.0))
    return jnp.clip(scales * (alignment * shared[:, None] + jitter), -250.0, 250.0)


def draw_center(key, part):
    trend = 0.08 * (1.0 - 2.0 * jnp.arange(K, dtype=jnp.float32) / K)
    value_key = jax.random.fold_in(key, 404)
    spread = 0.4 * jax.random.uniform(value_key, (K,), jnp.float32, -1.0, 1.0)
    return trend + spread


def block_levels(rng, dims, shards, smallest, high):
    level = 1.0
    for dim, shards_of in shards:
        heights = jax.random.uniform(jax.random.fold_in(jax.random.fold_in(rng, 6), dim), (shards_of,), jnp.float32, smallest / len(shards), high / len(shards))
        level = level * jnp.repeat(jnp.exp(heights), dims[dim] // shards_of).reshape((-1,) + (1,) * (len(dims) - 1 - dim))
    return level


def centred(rng, shape, width, reach, cuts=(), kind=jnp.bfloat16):
    drawn = width * jax.random.normal(rng, shape, jnp.float32)
    if cuts:
        drawn = drawn * block_levels(rng, shape, cuts, -0.22, 0.18)
    return jnp.clip(drawn, -reach, reach).astype(kind)


def setup_inputs(seed: int = 0) -> dict:
    keys = jax.random.split(jax.random.key(seed), 5)
    features = draw_features(jax.random.fold_in(keys[4], 71), 0)
    teacher_weight = draw_teacher_weight(jax.random.fold_in(keys[4], 71), 0)
    student_weight = centred(keys[2], (D, K), 4.0, 24.0, ((1, 512),), jnp.float32)
    center = draw_center(jax.random.fold_in(keys[4], 71), 0)
    return {"features": features, "teacher_weight": teacher_weight, "student_weight": student_weight, "center": center}


ema_momentum = 0.994
center_momentum = 0.9
teacher_temp = 0.07
epsilon = 1e-06

def reference(features, teacher_weight, student_weight, center):
    blended = ema_momentum * teacher_weight + (1.0 - ema_momentum) * student_weight
    col_norm = jnp.sqrt(lax.optimization_barrier(jnp.sum(blended * blended, axis=0, keepdims=True)) + epsilon)
    protos = (blended / col_norm).astype(jnp.bfloat16)
    wide_feats = features.astype(jnp.float32)
    row_norm = jnp.sqrt(lax.optimization_barrier(jnp.sum(wide_feats * wide_feats, axis=1, keepdims=True)) + epsilon)
    unit_rows = (wide_feats / row_norm).astype(jnp.bfloat16)
    logits = jnp.dot(unit_rows, protos, preferred_element_type=jnp.float32)
    column_sums = lax.optimization_barrier(jnp.sum(logits, axis=0))
    new_center = center_momentum * center + (1.0 - center_momentum) * (column_sums / IMAGES)
    shifted = (logits - new_center[None, :]) / teacher_temp
    totals = lax.optimization_barrier(jnp.sum(jnp.exp(shifted), axis=1))
    log_targets = shifted - jnp.log(totals)[:, None]
    return (blended, new_center, log_targets)
```

```python
import jax
import jax.numpy as jnp
from jax import lax
from jax.experimental import pallas as pl
from jax.experimental.pallas import tpu as pltpu
from jax.sharding import PartitionSpec as P

ema_momentum = 0.994
center_momentum = 0.9
teacher_temp = 0.07
epsilon = 1e-06

MESH = pl.DeviceIdType.MESH
NX, NY, NZ, NH = 4, 8, 8, 4
ROLES = 2 * NX
STEPS = (0, 1, 7, 2, 6, 3, 5, 4)


def gather_kernel(
    feat_ref, tw_ref, sw_ref, center_ref,
    scaled_ref, logs_ref, center_out_ref, blended_ref,
    rows, protos, part, role_buf, y_buf, z_buf, log_buf,
    recv_sem, z_send, y_send, x_send, relay_send, pair_send,
    role_recv, role_send, yb_recv, yb_send, zb_recv, zb_send, log_recv, log_send,
):
    dp = lax.axis_index("dp")
    mp = lax.axis_index("mp")
    core = lax.rem(dp, 2)
    y = lax.rem(lax.div(dp, 2), NY)
    zh = lax.div(dp, 2 * NY)
    x = lax.div(mp, 2)
    zl = lax.rem(mp, 2)
    z = zh * 2 + zl
    images = rows.shape[0] * rows.shape[1] * rows.shape[2] * rows.shape[3]

    def at(x_, y_, z_, c_):
        return ((lax.div(z_, 2) * NY + y_) * 2 + c_, x_ * 2 + lax.rem(z_, 2))

    def xs(k):
        return lax.rem(x + k, NX)

    def ys(k):
        return lax.rem(y + k, NY)

    def zs(k):
        return lax.rem(z + k, NZ)

    role = x * 2 + core

    def role_at(k):
        r = lax.rem(role + k, ROLES)
        return r, at(lax.div(r, 2), y, z, lax.rem(r, 2))

    barrier = pltpu.get_barrier_semaphore()
    for k in range(1, ROLES):
        pl.semaphore_signal(barrier, inc=1, device_id=role_at(k)[1], device_id_type=MESH)
    for k in range(1, NY):
        pl.semaphore_signal(barrier, inc=1, device_id=at(x, ys(k), z, core), device_id_type=MESH)
    for k in range(1, NZ):
        pl.semaphore_signal(barrier, inc=1, device_id=at(x, y, zs(k), core), device_id_type=MESH)

    source = zh == x

    @pl.when(source)
    def _():
        wide = feat_ref[...].astype(jnp.float32)
        norm = jnp.sqrt(jnp.sum(wide * wide, axis=1, keepdims=True) + epsilon)
        rows[x, y, core] = (wide / norm).astype(jnp.bfloat16)

    pl.semaphore_wait(barrier, ROLES + NY + NZ - 3)

    pending = []

    def send(slot, send_sem, target):
        copy = pltpu.make_async_remote_copy(
            src_ref=rows.at[slot],
            dst_ref=rows.at[slot],
            send_sem=send_sem,
            recv_sem=recv_sem.at[slot],
            device_id=target,
            device_id_type=MESH,
        )
        copy.start()
        pending.append(copy)

    def arrive(slot):
        pltpu.make_async_remote_copy(
            src_ref=rows.at[slot],
            dst_ref=rows.at[slot],
            send_sem=z_send.at[0],
            recv_sem=recv_sem.at[slot],
            device_id=at(x, y, z, 1 - core),
            device_id_type=MESH,
        ).wait_recv()

    def z_copy(k):
        slot = (x, y, core)
        step = jnp.where(zl == 1, k, NZ - k)
        return pltpu.make_async_remote_copy(
            src_ref=rows.at[slot],
            dst_ref=rows.at[slot],
            send_sem=z_send.at[k - 1],
            recv_sem=recv_sem.at[slot],
            device_id=at(x, y, zs(step), core),
            device_id_type=MESH,
        )

    @pl.when(source)
    def _():
        for k in range(1, 4):
            z_copy(k).start()

    blended = ema_momentum * tw_ref[...] + (1.0 - ema_momentum) * sw_ref[...]
    blended_ref[...] = blended
    col_norm = jnp.sqrt(jnp.sum(blended * blended, axis=0, keepdims=True) + epsilon)
    protos[...] = (blended / col_norm).astype(jnp.bfloat16)

    pair_count = [0]

    def to_pair(slot):
        send(slot, pair_send.at[pair_count[0]], at(x, y, z, 1 - core))
        pair_count[0] += 1

    def own_stage(i):
        slot = (x, ys(STEPS[i]), core)
        if i == 0:
            @pl.when(jnp.logical_not(source))
            def _():
                arrive(slot)

            for k in range(1, NY):
                send(slot, y_send.at[k - 1], at(x, ys(STEPS[k]), z, core))
        else:
            arrive(slot)
        send(slot, x_send.at[0, i], at(xs(1), y, z, core))
        send(slot, x_send.at[1, i], at(xs(NX - 1), y, z, core))
        to_pair(slot)

    def near_stage(i):
        yy = ys(STEPS[i])
        for k in (NX - 1, 1):
            slot = (xs(k), yy, core)
            arrive(slot)
            if (i % 2 == 0) == (k == 1):
                send(slot, relay_send.at[i], at(xs(NX - k), y, z, core))
            to_pair(slot)

    def far_stage(i):
        slot = (xs(2), ys(STEPS[i]), core)
        arrive(slot)
        to_pair(slot)

    for i in range(NY + 3):
        if i < NY:
            own_stage(i)
        if 1 <= i < NY + 1:
            near_stage(i - 1)
        if 3 <= i:
            far_stage(i - 3)

    sums = jnp.zeros((1, protos.shape[1]), jnp.float32)
    block = rows.shape[1] * rows.shape[2] * rows.shape[3]
    for k in (0, 1, 3, 2):
        group = xs(k)
        for i in range(NY):
            arrive((group, ys(STEPS[i]), 1 - core))
        lhs = rows[group].reshape(block, rows.shape[4])
        logits = jnp.dot(lhs, protos[...], preferred_element_type=jnp.float32)
        sums = sums + jnp.sum(logits, axis=0, keepdims=True)
        scaled_ref[group] = logits * (1.0 / teacher_temp)

    new_center = center_momentum * center_ref[...] + (1.0 - center_momentum) * (sums / images)
    center_out_ref[...] = new_center
    shift = new_center * (1.0 / teacher_temp)

    half = protos.shape[1] // 2
    each = images // ROLES
    ones = jnp.ones((8, 2 * half), jnp.bfloat16)
    for j in range(ROLES):
        group, start = j // 2, (j % 2) * each
        e = jnp.exp(scaled_ref[group, start:start + each, :] - shift)
        folded = e[:, :half] + e[:, half:]
        high = folded.astype(jnp.bfloat16)
        low = (folded - high.astype(jnp.float32)).astype(jnp.bfloat16)
        both = jnp.concatenate([high, low], axis=1)
        total = lax.dot_general(
            ones, both, (((1,), (1,)), ((), ())), preferred_element_type=jnp.float32
        )
        part[j] = total[0:1]

    def exchange(src, src_slot, dst, dst_slot, ssem, rsem, target):
        copy = pltpu.make_async_remote_copy(
            src_ref=src.at[src_slot],
            dst_ref=dst.at[dst_slot],
            send_sem=ssem,
            recv_sem=rsem,
            device_id=target,
            device_id_type=MESH,
        )
        copy.start()
        pending.append(copy)

    def landed(dst, slot, rsem, ssem):
        pltpu.make_async_remote_copy(
            src_ref=dst.at[slot],
            dst_ref=dst.at[slot],
            send_sem=ssem,
            recv_sem=rsem,
            device_id=at(x, y, z, 1 - core),
            device_id_type=MESH,
        ).wait_recv()

    for k in range(1, ROLES):
        r, target = role_at(k)
        exchange(part, r, role_buf, role, role_send.at[k - 1], role_recv.at[role], target)
    role_buf[role] = part[role]
    for k in range(1, ROLES):
        r, _ = role_at(k)
        landed(role_buf, r, role_recv.at[r], role_send.at[0])
    y_buf[y] = jnp.sum(role_buf[...], axis=0)

    for k in range(1, NY):
        exchange(y_buf, y, y_buf, y, yb_send.at[k - 1], yb_recv.at[y], at(x, ys(k), z, core))
    for k in range(1, NY):
        landed(y_buf, ys(k), yb_recv.at[ys(k)], yb_send.at[0])
    z_buf[z] = jnp.sum(y_buf[...], axis=0)

    for k in range(1, NZ):
        exchange(z_buf, z, z_buf, z, zb_send.at[k - 1], zb_recv.at[z], at(x, y, zs(k), core))
    for k in range(1, NZ):
        landed(z_buf, zs(k), zb_recv.at[zs(k)], zb_send.at[0])
    log_buf[role] = jnp.log(jnp.sum(z_buf[...], axis=0))

    for k in range(1, ROLES):
        _, target = role_at(k)
        exchange(log_buf, role, log_buf, role, log_send.at[k - 1], log_recv.at[role], target)
    for k in range(1, ROLES):
        r, _ = role_at(k)
        landed(log_buf, r, log_recv.at[r], log_send.at[0])
    logs_ref[...] = log_buf[...]

    @pl.when(source)
    def _():
        for k in range(1, 4):
            z_copy(k).wait_send()

    for copy in pending:
        copy.wait_send()


def write_kernel(scaled_ref, logs_ref, center_ref, blended_ref, out_ref, blended_out, center_out, stage, sem):
    early = (
        pltpu.make_async_copy(blended_ref, blended_out, sem.at[ROLES]),
        pltpu.make_async_copy(center_ref, center_out, sem.at[ROLES + 1]),
    )
    for copy in early:
        copy.start()
    shift = center_ref[...] * (1.0 / teacher_temp)
    each = stage.shape[1]
    copies = []
    for j in range(ROLES):
        group, start = j // 2, (j % 2) * each
        for i in range(each // 128):
            row = logs_ref[j, :, i * 128:(i + 1) * 128]
            column = jnp.broadcast_to(row, (128, 128)).T
            both = jnp.concatenate([column, column], axis=1)
            there = slice(start + i * 128, start + (i + 1) * 128)
            stage[j, i * 128:(i + 1) * 128, :] = (scaled_ref[group, there, :] - shift) - both
        copy = pltpu.make_async_copy(stage.at[j], out_ref.at[pl.ds(j * each, each)], sem.at[j])
        copy.start()
        copies.append(copy)
    for copy in copies:
        copy.wait()
    for copy in early:
        copy.wait()


def shards(features, teacher_weight, student_weight, center):
    rows_here, depth = features.shape
    width = teacher_weight.shape[1]
    images = rows_here * lax.axis_size("dp")
    each = images // ROLES
    vmem = pl.BlockSpec(memory_space=pltpu.VMEM)
    anywhere = pl.BlockSpec(memory_space=pl.ANY)
    f32 = jnp.float32
    dma = pltpu.SemaphoreType.DMA
    small = lambda n: pltpu.VMEM((n, 1, each), f32)
    scaled, logs, new_center, blended = pl.pallas_call(
        gather_kernel,
        out_shape=(
            jax.ShapeDtypeStruct((NH, images // NH, width), f32),
            jax.ShapeDtypeStruct((ROLES, 1, each), f32),
            jax.ShapeDtypeStruct((1, width), f32),
            jax.ShapeDtypeStruct((depth, width), f32),
        ),
        in_specs=[vmem] * 4,
        out_specs=[vmem] * 4,
        scratch_shapes=[
            pltpu.VMEM((NH, NY, 2, rows_here, depth), jnp.bfloat16),
            pltpu.VMEM((depth, width), jnp.bfloat16),
            small(ROLES), small(ROLES), small(NY), small(NZ), small(ROLES),
            dma((NH, NY, 2)), dma((3,)), dma((NY - 1,)), dma((2, NY)), dma((NY,)), dma((NH * NY,)),
            dma((ROLES,)), dma((ROLES - 1,)), dma((NY,)), dma((NY - 1,)),
            dma((NZ,)), dma((NZ - 1,)), dma((ROLES,)), dma((ROLES - 1,)),
        ],
        compiler_params=pltpu.CompilerParams(collective_id=0, has_side_effects=True),
        name="gather",
    )(features, teacher_weight, student_weight, center.reshape(1, width))
    log_targets, blended, new_center = pl.pallas_call(
        write_kernel,
        out_shape=(
            jax.ShapeDtypeStruct((images, width), f32),
            jax.ShapeDtypeStruct((depth, width), f32),
            jax.ShapeDtypeStruct((1, width), f32),
        ),
        in_specs=[vmem] * 4,
        out_specs=[anywhere] * 3,
        scratch_shapes=[pltpu.VMEM((ROLES, each, width), f32), dma((ROLES + 2,))],
        name="write",
    )(scaled, logs, new_center, blended)
    return (blended, new_center.reshape(width), log_targets)


def solution(mesh):
    placed = (P("dp", None), P(None, ("dp", "mp")), P(None, ("dp", "mp")), P(("dp", "mp")))
    return jax.shard_map(
        shards,
        mesh=mesh,
        in_specs=placed,
        out_specs=(P(None, ("dp", "mp")), P(("dp", "mp")), P(None, ("dp", "mp"))),
        check_vma=False,
    )
```

```python
import jax
import jax.numpy as jnp
from jax import lax
from jax.experimental import pallas as pl
from jax.experimental.pallas import tpu as pltpu
from jax.sharding import PartitionSpec as P

ema_momentum = 0.994
center_momentum = 0.9
teacher_temp = 0.07
epsilon = 1e-06

MESH = pl.DeviceIdType.MESH
NX, NY, NZ, NH = 4, 8, 8, 4
ROLES = 2 * NX
STEPS = (0, 1, 7, 2, 6, 3, 5, 4)


def gather_kernel(
    feat_hbm, tw_hbm, sw_hbm, center_hbm,
    scaled_ref, logs_ref, center_out_ref, blended_ref,
    feat, student, center, rows, protos, part, role_buf, y_buf, z_buf, log_buf,
    load_sem, recv_sem, z_send, y_send, cross_send, pair_send,
    role_recv, role_send, yb_recv, yb_send, zb_recv, zb_send, log_recv, log_send,
):
    dp = lax.axis_index("dp")
    mp = lax.axis_index("mp")
    core = lax.rem(dp, 2)
    y = lax.rem(lax.div(dp, 2), NY)
    zh = lax.div(dp, 2 * NY)
    x = lax.div(mp, 2)
    zl = lax.rem(mp, 2)
    z = zh * 2 + zl
    images = rows.shape[0] * rows.shape[1] * rows.shape[2] * rows.shape[3]

    def at(x_, y_, z_, c_):
        return ((lax.div(z_, 2) * NY + y_) * 2 + c_, x_ * 2 + lax.rem(z_, 2))

    def xs(k):
        return lax.rem(x + k, NX)

    def ys(k):
        return lax.rem(y + k, NY)

    def zs(k):
        return lax.rem(z + k, NZ)

    role = x * 2 + core

    def role_at(k):
        r = lax.rem(role + k, ROLES)
        return r, at(lax.div(r, 2), y, z, lax.rem(r, 2))

    pair = at(x, y, z, 1 - core)

    barrier = pltpu.get_barrier_semaphore()
    for k in range(1, NZ):
        pl.semaphore_signal(barrier, inc=1, device_id=at(x, y, zs(k), core), device_id_type=MESH)
    for k in range(1, NY):
        pl.semaphore_signal(barrier, inc=1, device_id=at(x, ys(k), z, core), device_id_type=MESH)
    for k in range(1, ROLES):
        pl.semaphore_signal(barrier, inc=1, device_id=role_at(k)[1], device_id_type=MESH)

    loads = [
        pltpu.make_async_copy(feat_hbm, feat, load_sem.at[0]),
        pltpu.make_async_copy(tw_hbm, blended_ref, load_sem.at[1]),
        pltpu.make_async_copy(sw_hbm, student, load_sem.at[2]),
        pltpu.make_async_copy(center_hbm, center, load_sem.at[3]),
    ]
    for load in loads:
        load.start()

    spread_x = core == 1
    base = jnp.where(spread_x, x, zh)
    source = jnp.logical_or(core == 0, zh == x)
    fetched = jnp.logical_and(core == 1, zh == x)
    sign = jnp.where(zl == 1, 1, NZ - 1)

    loads[0].wait()

    @pl.when(source)
    def _():
        wide = feat[...].astype(jnp.float32)
        norm = jnp.sqrt(jnp.sum(wide * wide, axis=1, keepdims=True) + epsilon)
        rows[base, y, core] = (wide / norm).astype(jnp.bfloat16)

    with jax.named_scope("barrier"):
        pl.semaphore_wait(barrier, ROLES + NY + NZ - 3)

    pending = []

    def block_copy(slot, send_sem, target):
        return pltpu.make_async_remote_copy(
            src_ref=rows.at[slot],
            dst_ref=rows.at[slot],
            send_sem=send_sem,
            recv_sem=recv_sem.at[slot],
            device_id=target,
            device_id_type=MESH,
        )

    def send(slot, send_sem, target):
        copy = block_copy(slot, send_sem, target)
        copy.start()
        pending.append(copy)

    def arrive(slot):
        block_copy(slot, z_send.at[0], pair).wait_recv()

    def z_target(k):
        return zs(lax.rem(sign * k, NZ))

    def z_copy(k):
        return block_copy((base, y, core), z_send.at[k - 1], at(x, y, z_target(k), core))

    @pl.when(fetched)
    def _():
        for k in range(1, NH):
            z_copy(k).start()

    pair_count = [0]

    def to_pair(slot):
        send(slot, pair_send.at[pair_count[0]], pair)
        pair_count[0] += 1

    def spread(slot, i):
        for n, k in enumerate((1, 3, 2)):
            k_z = n + 1
            target = at(
                jnp.where(spread_x, xs(k), x), y, jnp.where(spread_x, z, z_target(k_z)), core
            )
            send(slot, cross_send.at[n, i], target)
        to_pair(slot)

    def own_stage(i):
        slot = (base, ys(STEPS[i]), core)
        if i == 0:
            @pl.when(jnp.logical_not(source))
            def _():
                arrive(slot)

            for k in range(1, NY):
                send(slot, y_send.at[k - 1], at(x, ys(STEPS[k]), z, core))
        else:
            arrive(slot)
        spread(slot, i)

    def cross_stage(i):
        for k in (1, 3, 2):
            slot = (lax.rem(base + k, NH), ys(STEPS[i]), core)
            arrive(slot)
            to_pair(slot)

    with jax.named_scope("own0"):
        own_stage(0)

    loads[1].wait()
    loads[2].wait()
    blended = ema_momentum * blended_ref[...] + (1.0 - ema_momentum) * student[...]
    blended_ref[...] = blended
    col_norm = jnp.sqrt(jnp.sum(blended * blended, axis=0, keepdims=True) + epsilon)
    protos[...] = (blended / col_norm).astype(jnp.bfloat16)

    for i in range(1, NY):
        with jax.named_scope(f"own{i}"):
            own_stage(i)

    sums = [jnp.zeros((1, protos.shape[1]), jnp.float32)]

    def dot_stage(i):
        yy = ys(STEPS[i])
        with jax.named_scope(f"pair{i}"):
            for group in range(NH):
                arrive((group, yy, 1 - core))
        lhs = rows[:, yy].reshape(NH * 2 * rows.shape[3], rows.shape[4])
        logits = jnp.dot(lhs, protos[...], preferred_element_type=jnp.float32)
        sums[0] = sums[0] + jnp.sum(logits, axis=0, keepdims=True)
        scaled = logits * (1.0 / teacher_temp)
        scaled_ref[:, yy] = scaled.reshape(NH, 2 * rows.shape[3], protos.shape[1])

    for i in range(NY):
        with jax.named_scope(f"cross{i}"):
            cross_stage(i)
        if i >= 1:
            dot_stage(i - 1)
    dot_stage(NY - 1)

    loads[3].wait()
    new_center = center_momentum * center[...] + (1.0 - center_momentum) * (sums[0] / images)
    center_out_ref[...] = new_center
    shift = new_center * (1.0 / teacher_temp)

    half = protos.shape[1] // 2
    pieces = 4
    each = images // (2 * pieces)
    ones = jnp.ones((8, 2 * half), jnp.bfloat16)
    for j in range(2 * pieces):
        group, start = j // 2, (j % 2) * (NY // 2)
        e = jnp.exp(scaled_ref[group, start:start + NY // 2] - shift).reshape(each, 2 * half)
        folded = e[:, :half] + e[:, half:]
        high = folded.astype(jnp.bfloat16)
        low = (folded - high.astype(jnp.float32)).astype(jnp.bfloat16)
        both = jnp.concatenate([high, low], axis=1)
        total = lax.dot_general(
            ones, both, (((1,), (1,)), ((), ())), preferred_element_type=jnp.float32
        )
        where = (j % pieces) * each
        part[j // pieces, :, where:where + each] = total[0:1]

    def exchange(src, src_slot, dst, dst_slot, ssem, rsem, target):
        copy = pltpu.make_async_remote_copy(
            src_ref=src.at[src_slot],
            dst_ref=dst.at[dst_slot],
            send_sem=ssem,
            recv_sem=rsem,
            device_id=target,
            device_id_type=MESH,
        )
        copy.start()
        pending.append(copy)

    def landed(dst, slot, rsem, ssem):
        pltpu.make_async_remote_copy(
            src_ref=dst.at[slot],
            dst_ref=dst.at[slot],
            send_sem=ssem,
            recv_sem=rsem,
            device_id=pair,
            device_id_type=MESH,
        ).wait_recv()

    with jax.named_scope("role"):
        for k in range(1, ROLES):
            r, target = role_at(k)
            exchange(
                part, lax.rem(r, 2), role_buf, role, role_send.at[k - 1], role_recv.at[role], target
            )
        role_buf[role] = part[core]
        for k in range(1, ROLES):
            r, _ = role_at(k)
            landed(role_buf, r, role_recv.at[r], role_send.at[0])
        y_buf[y] = jnp.sum(role_buf[...], axis=0)

    with jax.named_scope("ysum"):
        for k in range(1, NY):
            exchange(y_buf, y, y_buf, y, yb_send.at[k - 1], yb_recv.at[y], at(x, ys(k), z, core))
        for k in range(1, NY):
            landed(y_buf, ys(k), yb_recv.at[ys(k)], yb_send.at[0])
        z_buf[z] = jnp.sum(y_buf[...], axis=0)

    with jax.named_scope("zsum"):
        for k in range(1, NZ):
            exchange(z_buf, z, z_buf, z, zb_send.at[k - 1], zb_recv.at[z], at(x, y, zs(k), core))
        for k in range(1, NZ):
            landed(z_buf, zs(k), zb_recv.at[zs(k)], zb_send.at[0])
        log_buf[core] = jnp.log(jnp.sum(z_buf[...], axis=0))

    with jax.named_scope("log"):
        exchange(log_buf, core, log_buf, core, log_send.at[0], log_recv.at[core], pair)
        landed(log_buf, 1 - core, log_recv.at[1 - core], log_send.at[0])
        logs_ref[...] = log_buf[...]

    with jax.named_scope("drain"):
        @pl.when(fetched)
        def _():
            for k in range(1, NH):
                z_copy(k).wait_send()

        for copy in pending:
            copy.wait_send()


def write_kernel(scaled_ref, logs_ref, center_ref, blended_ref, out_ref, blended_out, center_out, stage, sem):
    pieces = stage.shape[0]
    early = (
        pltpu.make_async_copy(blended_ref, blended_out, sem.at[pieces]),
        pltpu.make_async_copy(center_ref, center_out, sem.at[pieces + 1]),
    )
    for copy in early:
        copy.start()
    shift = center_ref[...] * (1.0 / teacher_temp)
    each, width = stage.shape[1:]
    copies = []
    for j in range(pieces):
        group, start = j // 2, (j % 2) * (NY // 2)
        scaled = scaled_ref[group, start:start + NY // 2].reshape(each, width)
        where = (j % (pieces // 2)) * each
        for i in range(each // 128):
            row = logs_ref[j // (pieces // 2), :, where + i * 128:where + (i + 1) * 128]
            column = jnp.broadcast_to(row, (128, 128)).T
            both = jnp.concatenate([column, column], axis=1)
            there = slice(i * 128, (i + 1) * 128)
            stage[j, there, :] = (scaled[there, :] - shift) - both
        copy = pltpu.make_async_copy(stage.at[j], out_ref.at[pl.ds(j * each, each)], sem.at[j])
        copy.start()
        copies.append(copy)
    for copy in copies:
        copy.wait()
    for copy in early:
        copy.wait()


def shards(features, teacher_weight, student_weight, center):
    rows_here, depth = features.shape
    width = teacher_weight.shape[1]
    images = rows_here * lax.axis_size("dp")
    vmem = pl.BlockSpec(memory_space=pltpu.VMEM)
    anywhere = pl.BlockSpec(memory_space=pl.ANY)
    f32 = jnp.float32
    dma = pltpu.SemaphoreType.DMA
    halves = lambda n: pltpu.VMEM((n, 1, images // 2), f32)
    results = pl.pallas_call(
        gather_kernel,
        out_shape=(
            pltpu.VMEM((NH, NY, 2 * rows_here, width), f32),
            halves(2),
            pltpu.VMEM((1, width), f32),
            pltpu.VMEM((depth, width), f32),
        ),
        in_specs=[anywhere] * 4,
        out_specs=[vmem] * 4,
        scratch_shapes=[
            pltpu.VMEM((rows_here, depth), jnp.bfloat16),
            pltpu.VMEM((depth, width), f32),
            pltpu.VMEM((1, width), f32),
            pltpu.VMEM((NH, NY, 2, rows_here, depth), jnp.bfloat16),
            pltpu.VMEM((depth, width), jnp.bfloat16),
            halves(2), halves(ROLES), halves(NY), halves(NZ), halves(2),
            dma((4,)), dma((NH, NY, 2)), dma((NH - 1,)), dma((NY - 1,)), dma((3, NY)), dma((NH * NY,)),
            dma((ROLES,)), dma((ROLES - 1,)), dma((NY,)), dma((NY - 1,)),
            dma((NZ,)), dma((NZ - 1,)), dma((2,)), dma((1,)),
        ],
        compiler_params=pltpu.CompilerParams(collective_id=0, has_side_effects=True),
        name="gather",
    )(features, teacher_weight, student_weight, center.reshape(1, width))
    results = [pltpu.with_memory_space_constraint(r, pltpu.VMEM) for r in results]
    pieces = 8
    log_targets, blended, new_center = pl.pallas_call(
        write_kernel,
        out_shape=(
            jax.ShapeDtypeStruct((images, width), f32),
            jax.ShapeDtypeStruct((depth, width), f32),
            jax.ShapeDtypeStruct((1, width), f32),
        ),
        in_specs=[vmem] * 4,
        out_specs=[anywhere] * 3,
        scratch_shapes=[pltpu.VMEM((pieces, images // pieces, width), f32), dma((pieces + 2,))],
        name="write",
    )(*results)
    return (blended, new_center.reshape(width), log_targets)


def solution(mesh):
    placed = (P("dp", None), P(None, ("dp", "mp")), P(None, ("dp", "mp")), P(("dp", "mp")))
    return jax.shard_map(
        shards,
        mesh=mesh,
        in_specs=placed,
        out_specs=(P(None, ("dp", "mp")), P(("dp", "mp")), P(None, ("dp", "mp"))),
        check_vma=False,
    )
```

```python
import jax
import jax.numpy as jnp
from jax import lax
from jax.experimental import pallas as pl
from jax.experimental.pallas import tpu as pltpu
from jax.sharding import PartitionSpec as P

ema_momentum = 0.994
center_momentum = 0.9
teacher_temp = 0.07
epsilon = 1e-06

MESH = pl.DeviceIdType.MESH
NX, NY, NZ, NH = 4, 8, 8, 4
ROLES = 2 * NX
STEPS = (0, 1, 7, 2, 6, 3, 5, 4)


def gather_kernel(
    feat_hbm, tw_hbm, sw_hbm, center_hbm,
    scaled_ref, logs_ref, center_out_ref, blended_ref,
    feat, student, center, rows, protos, part, role_buf, y_buf, z_buf, log_buf,
    load_sem, known_sem, own_recv, near_recv, rest_recv, pair_recv,
    z_send, y_send, cross_send, pair_send, sum_recv, sum_send,
):
    dp = lax.axis_index("dp")
    mp = lax.axis_index("mp")
    core = lax.rem(dp, 2)
    y = lax.rem(lax.div(dp, 2), NY)
    zh = lax.div(dp, 2 * NY)
    x = lax.div(mp, 2)
    zl = lax.rem(mp, 2)
    z = zh * 2 + zl
    images = rows.shape[0] * rows.shape[1] * rows.shape[2] * rows.shape[3]

    def at(x_, y_, z_, c_):
        return ((lax.div(z_, 2) * NY + y_) * 2 + c_, x_ * 2 + lax.rem(z_, 2))

    def xs(k):
        return lax.rem(x + k, NX)

    def ys(k):
        return lax.rem(y + k, NY)

    def zs(k):
        return lax.rem(z + k, NZ)

    role = x * 2 + core

    def role_at(k):
        r = lax.rem(role + k, ROLES)
        return r, at(lax.div(r, 2), y, z, lax.rem(r, 2))

    pair = at(x, y, z, 1 - core)

    twice = [at(x, ys(2), z, core), at(x, ys(NY - 2), z, core), at(x, y, zs(2), core), at(x, y, zs(NZ - 2), core)]
    close = [at(x, ys(1), z, core), at(x, ys(NY - 1), z, core), at(x, y, zs(1), core), at(x, y, zs(NZ - 1), core)]
    close += [pair] + twice + [at(xs(k), y, z, core) for k in range(1, NX)]

    barrier = pltpu.get_barrier_semaphore()
    for peer in close:
        pl.semaphore_signal(barrier, inc=1, device_id=peer, device_id_type=MESH)

    loads = [
        pltpu.make_async_copy(feat_hbm, feat, load_sem.at[0]),
        pltpu.make_async_copy(tw_hbm, blended_ref, load_sem.at[1]),
        pltpu.make_async_copy(sw_hbm, student, load_sem.at[2]),
        pltpu.make_async_copy(center_hbm, center, load_sem.at[3]),
    ]
    for load in loads:
        load.start()

    spread_x = core == 1
    base = jnp.where(spread_x, x, zh)
    source = jnp.logical_or(core == 0, zh == x)
    fetched = jnp.logical_and(core == 1, zh == x)
    ahead = lax.rem(zh - x + NH, NH)
    passed_on = jnp.logical_and(core == 1, ahead == jnp.where(zl == 1, 1, NH - 1))
    sign = jnp.where(zl == 1, 1, NZ - 1)

    with jax.named_scope("load"):
        loads[0].wait()

    @pl.when(source)
    def _():
        wide = feat[...].astype(jnp.float32)
        norm = jnp.sqrt(jnp.sum(wide * wide, axis=1, keepdims=True) + epsilon)
        rows[base, y, core] = (wide / norm).astype(jnp.bfloat16)

    with jax.named_scope("barrier"):
        pl.semaphore_wait(barrier, len(close))
    for peer in twice + [pair]:
        pl.semaphore_signal(known_sem, inc=1, device_id=peer, device_id_type=MESH)

    def block_copy(slot, send_sem, recv_sem, target):
        return pltpu.make_async_remote_copy(
            src_ref=rows.at[slot],
            dst_ref=rows.at[slot],
            send_sem=send_sem,
            recv_sem=recv_sem,
            device_id=target,
            device_id_type=MESH,
        )

    def sized(blocks, sem):
        return pltpu.make_async_remote_copy(
            src_ref=blocks, dst_ref=blocks, send_sem=sem, recv_sem=sem, device_id=pair, device_id_type=MESH
        )

    def one_block():
        return rows.at[base, y, core]

    def z_target(k):
        return zs(lax.rem(sign * k, NZ))

    def z_copy(k):
        return block_copy((base, y, core), z_send, own_recv.at[y], at(x, y, z_target(k), core))

    @pl.when(fetched)
    def _():
        for k in (1, 2):
            z_copy(k).start()

    def to_pair(slot):
        block_copy(slot, pair_send, pair_recv.at[slot[1]], pair).start()

    def y_copy(slot, k):
        block_copy(slot, y_send, own_recv.at[slot[1]], at(x, ys(k), z, core)).start()

    def x_copy(slot, k, sem):
        block_copy(slot, cross_send, sem.at[slot[1]], at(xs(k), y, z, core)).start()

    def own_stage(i):
        step = STEPS[i]
        yy = ys(step)
        slot = (base, yy, core)
        if i == 0:
            @pl.when(jnp.logical_not(source))
            def _():
                sized(one_block(), own_recv.at[yy]).wait_recv()

            @pl.when(passed_on)
            def _():
                z_copy(1).start()

            for k in (1, NY - 1, 2, NY - 2):
                y_copy(slot, k)
        else:
            sized(one_block(), own_recv.at[yy]).wait_recv()
        if step == 2:
            y_copy(slot, NY - 1)
        if step == NY - 2:
            y_copy(slot, 1)
            back = jnp.where(spread_x, 2, NY - 2)
            y_copy((base, ys(back), core), NY - back)

        @pl.when(spread_x)
        def _():
            x_copy(slot, NX - 1, near_recv)
            x_copy(slot, 1, rest_recv)
            x_copy(slot, 2, rest_recv)

        @pl.when(jnp.logical_not(spread_x))
        def _():
            block_copy(slot, cross_send, near_recv.at[yy], at(x, y, z_target(1), core)).start()

        to_pair(slot)

    turns = (jnp.where(spread_x, 1, jnp.where(zl == 1, 1, 3)), jnp.where(spread_x, 3, jnp.where(zl == 1, 3, 1)), 2)

    def cross_slot(i, n):
        return (lax.rem(base + turns[n], NH), ys(STEPS[i]), core)

    def near_stage(i):
        slot = cross_slot(i, 0)
        sized(one_block(), near_recv.at[slot[1]]).wait_recv()

        @pl.when(jnp.logical_not(spread_x))
        def _():
            for k in (NZ - 1, NZ - 2):
                block_copy(slot, cross_send, rest_recv.at[slot[1]], at(x, y, z_target(k), core)).start()

        to_pair(slot)

    def rest_stage(i):
        yy = ys(STEPS[i])
        sized(rows.at[pl.ds(0, 2), yy, core], rest_recv.at[yy]).wait_recv()
        for n in (1, 2):
            to_pair(cross_slot(i, n))

    with jax.named_scope("own0"):
        own_stage(0)

    loads[1].wait()
    loads[2].wait()
    blended = ema_momentum * blended_ref[...] + (1.0 - ema_momentum) * student[...]
    blended_ref[...] = blended
    col_norm = jnp.sqrt(jnp.sum(blended * blended, axis=0, keepdims=True) + epsilon)
    protos[...] = (blended / col_norm).astype(jnp.bfloat16)

    sums = [jnp.zeros((1, protos.shape[1]), jnp.float32)]

    def dot_stage(i):
        yy = ys(STEPS[i])
        sized(rows.at[:, yy, 1 - core], pair_recv.at[yy]).wait_recv()
        lhs = rows[:, yy].reshape(NH * 2 * rows.shape[3], rows.shape[4])
        logits = jnp.dot(lhs, protos[...], preferred_element_type=jnp.float32)
        sums[0] = sums[0] + jnp.sum(logits, axis=0, keepdims=True)
        scaled = logits * (1.0 / teacher_temp)
        scaled_ref[:, yy] = scaled.reshape(NH, 2 * rows.shape[3], protos.shape[1])

    stages = {"own": own_stage, "near": near_stage, "rest": rest_stage, "dot": dot_stage}
    order = (
        ("own", (1, 2)), ("near", (0,)), ("own", (3, 4)), ("near", (1, 2)), ("rest", (0,)), ("own", (5, 6)),
        ("near", (3, 4)), ("own", (7,)), ("near", (5, 6)), ("rest", (1, 2)), ("dot", (0,)), ("near", (7,)),
        ("rest", (3, 4)), ("dot", (1, 2)), ("rest", (5, 6)), ("dot", (3, 4)),
        ("rest", (7,)), ("dot", (5, 6, 7)),
    )
    for name, steps in order:
        for i in steps:
            with jax.named_scope(f"{name}{i}"):
                stages[name](i)

    loads[3].wait()
    new_center = center_momentum * center[...] + (1.0 - center_momentum) * (sums[0] / images)
    center_out_ref[...] = new_center
    shift = new_center * (1.0 / teacher_temp)

    half = protos.shape[1] // 2
    pieces = 4
    each = images // (2 * pieces)
    ones = jnp.ones((8, 2 * half), jnp.bfloat16)
    for j in range(2 * pieces):
        group, start = j // 2, (j % 2) * (NY // 2)
        e = jnp.exp(scaled_ref[group, start:start + NY // 2] - shift).reshape(each, 2 * half)
        folded = e[:, :half] + e[:, half:]
        high = folded.astype(jnp.bfloat16)
        low = (folded - high.astype(jnp.float32)).astype(jnp.bfloat16)
        both = jnp.concatenate([high, low], axis=1)
        total = lax.dot_general(
            ones, both, (((1,), (1,)), ((), ())), preferred_element_type=jnp.float32
        )
        where = (j % pieces) * each
        part[j // pieces, :, where:where + each] = total[0:1]

    def exchange(src, dst, ssem, rsem, target):
        pltpu.make_async_remote_copy(
            src_ref=src, dst_ref=dst, send_sem=ssem, recv_sem=rsem, device_id=target, device_id_type=MESH
        ).start()

    with jax.named_scope("known"):
        pl.semaphore_wait(known_sem, len(twice) + 1)
    with jax.named_scope("role"):
        for k in range(1, ROLES):
            r, target = role_at(k)
            exchange(part.at[lax.rem(r, 2)], role_buf.at[role], sum_send.at[0], sum_recv.at[0], target)
        role_buf[role] = part[core]
        sized(role_buf.at[pl.ds(0, ROLES - 1)], sum_recv.at[0]).wait_recv()
        y_buf[y] = jnp.sum(role_buf[...], axis=0)

    with jax.named_scope("ysum"):
        for k in range(1, NY):
            exchange(y_buf.at[y], y_buf.at[y], sum_send.at[1], sum_recv.at[1], at(x, ys(k), z, core))
        sized(y_buf.at[pl.ds(0, NY - 1)], sum_recv.at[1]).wait_recv()
        z_buf[z] = jnp.sum(y_buf[...], axis=0)

    with jax.named_scope("zsum"):
        for k in range(1, NZ):
            exchange(z_buf.at[z], z_buf.at[z], sum_send.at[2], sum_recv.at[2], at(x, y, zs(k), core))
        sized(z_buf.at[pl.ds(0, NZ - 1)], sum_recv.at[2]).wait_recv()
        log_buf[core] = jnp.log(jnp.sum(z_buf[...], axis=0))

    with jax.named_scope("log"):
        exchange(log_buf.at[core], log_buf.at[core], sum_send.at[3], sum_recv.at[3], pair)
        sized(log_buf.at[core], sum_recv.at[3]).wait_recv()
        logs_ref[...] = log_buf[...]

    with jax.named_scope("drain"):
        @pl.when(fetched)
        def _():
            sized(rows.at[0, pl.ds(0, 2), core], z_send).wait_send()

        @pl.when(passed_on)
        def _():
            sized(one_block(), z_send).wait_send()

        sized(rows.at[0, pl.ds(0, NY - 1), core], y_send).wait_send()
        sized(rows.at[pl.ds(0, 3), :, core], cross_send).wait_send()
        sized(rows.at[:, :, core], pair_send).wait_send()
        sized(role_buf.at[pl.ds(0, ROLES - 1)], sum_send.at[0]).wait_send()
        sized(y_buf.at[pl.ds(0, NY - 1)], sum_send.at[1]).wait_send()
        sized(z_buf.at[pl.ds(0, NZ - 1)], sum_send.at[2]).wait_send()
        sized(log_buf.at[core], sum_send.at[3]).wait_send()


def write_kernel(scaled_ref, logs_ref, center_ref, blended_ref, out_ref, blended_out, center_out, stage, sem):
    pieces = stage.shape[0]
    early = (
        pltpu.make_async_copy(blended_ref, blended_out, sem.at[pieces]),
        pltpu.make_async_copy(center_ref, center_out, sem.at[pieces + 1]),
    )
    for copy in early:
        copy.start()
    shift = center_ref[...] * (1.0 / teacher_temp)
    each, width = stage.shape[1:]
    copies = []
    for j in range(pieces):
        group, start = j // 2, (j % 2) * (NY // 2)
        scaled = scaled_ref[group, start:start + NY // 2].reshape(each, width)
        where = (j % (pieces // 2)) * each
        for i in range(each // 128):
            row = logs_ref[j // (pieces // 2), :, where + i * 128:where + (i + 1) * 128]
            column = jnp.broadcast_to(row, (128, 128)).T
            both = jnp.concatenate([column, column], axis=1)
            there = slice(i * 128, (i + 1) * 128)
            stage[j, there, :] = (scaled[there, :] - shift) - both
        copy = pltpu.make_async_copy(stage.at[j], out_ref.at[pl.ds(j * each, each)], sem.at[j])
        copy.start()
        copies.append(copy)
    for copy in copies:
        copy.wait()
    for copy in early:
        copy.wait()


def shards(features, teacher_weight, student_weight, center):
    rows_here, depth = features.shape
    width = teacher_weight.shape[1]
    images = rows_here * lax.axis_size("dp")
    vmem = pl.BlockSpec(memory_space=pltpu.VMEM)
    anywhere = pl.BlockSpec(memory_space=pl.ANY)
    f32 = jnp.float32
    dma = pltpu.SemaphoreType.DMA
    halves = lambda n: pltpu.VMEM((n, 1, images // 2), f32)
    results = pl.pallas_call(
        gather_kernel,
        out_shape=(
            pltpu.VMEM((NH, NY, 2 * rows_here, width), f32),
            halves(2),
            pltpu.VMEM((1, width), f32),
            pltpu.VMEM((depth, width), f32),
        ),
        in_specs=[anywhere] * 4,
        out_specs=[vmem] * 4,
        scratch_shapes=[
            pltpu.VMEM((rows_here, depth), jnp.bfloat16),
            pltpu.VMEM((depth, width), f32),
            pltpu.VMEM((1, width), f32),
            pltpu.VMEM((NH, NY, 2, rows_here, depth), jnp.bfloat16),
            pltpu.VMEM((depth, width), jnp.bfloat16),
            halves(2), halves(ROLES), halves(NY), halves(NZ), halves(2),
            dma((4,)), pltpu.SemaphoreType.REGULAR, dma((NY,)), dma((NY,)), dma((NY,)), dma((NY,)),
            dma, dma, dma, dma, dma((4,)), dma((4,)),
        ],
        compiler_params=pltpu.CompilerParams(collective_id=0, has_side_effects=True),
        name="gather",
    )(features, teacher_weight, student_weight, center.reshape(1, width))
    results = [pltpu.with_memory_space_constraint(r, pltpu.VMEM) for r in results]
    pieces = 8
    log_targets, blended, new_center = pl.pallas_call(
        write_kernel,
        out_shape=(
            jax.ShapeDtypeStruct((images, width), f32),
            jax.ShapeDtypeStruct((depth, width), f32),
            jax.ShapeDtypeStruct((1, width), f32),
        ),
        in_specs=[vmem] * 4,
        out_specs=[anywhere] * 3,
        scratch_shapes=[pltpu.VMEM((pieces, images // pieces, width), f32), dma((pieces + 2,))],
        name="write",
    )(*results)
    return (blended, new_center.reshape(width), log_targets)


def solution(mesh):
    placed = (P("dp", None), P(None, ("dp", "mp")), P(None, ("dp", "mp")), P(("dp", "mp")))
    return jax.shard_map(
        shards,
        mesh=mesh,
        in_specs=placed,
        out_specs=(P(None, ("dp", "mp")), P(("dp", "mp")), P(None, ("dp", "mp"))),
        check_vma=False,
    )
```
